8 devices in a mesh: dp: 1 (over z), ep: 8 (over x, y, core).
Axes of the slice: x: 2, y: 2, z: 1, core: 2. Of those that a mesh axis runs over, the one named last changes fastest.
Arguments:
- x: bfloat16 [1, 8, 256, 5120], P('dp', 'ep')
- expert: int32 [1, 8, 256, 6], P('dp', 'ep')
- slot: int32 [1, 8, 256, 6], P('dp', 'ep')
- gate: float32 [1, 8, 256, 6], P('dp', 'ep')
- w_gate: bfloat16 [40, 5120, 1536], P('ep')
- w_up: bfloat16 [40, 5120, 1536], P('ep')
- w_down: bfloat16 [40, 1536, 5120], P('ep')
- s_gate: bfloat16 [5120, 3072], replicated
- s_up: bfloat16 [5120, 3072], replicated
- s_down: bfloat16 [3072, 5120], replicated
Outputs:
- y: bfloat16 [1, 8, 256, 5120], P('dp', 'ep')
All inputs are finite; a program needn't handle non-finite values.
Results may differ from the reference program's by a relative error of at most 0.009.
Values are sent between devices in bfloat16 or wider.
A program may use at most 2 GiB of HBM per device.

```python
import jax
import jax.numpy as jnp

MEMBERS = 8
TOKENS = 256
D = 5120
FF = 1536
TOP = 6
EXPERTS = 40
SHARED_FF = 3072
SLOTS = 5 * TOKENS * TOP // (4 * EXPERTS)


def setup_inputs(seed: int = 0, part: int = 0) -> dict:
    own, k1, k2, k3, k4, k5, k6 = jax.random.split(jax.random.key(seed), 7)
    kx, ke, kl, kg = jax.random.split(jax.random.fold_in(own, part), 4)
    devices = (1, MEMBERS)
    place = jax.random.permutation(kl, jnp.arange(EXPERTS, dtype=jnp.uint32))
    slow = ((EXPERTS + (9 * place) % EXPERTS) << ((9 * place) // EXPERTS)) // EXPERTS
    wait = (jax.random.bits(ke, (*devices, TOKENS, EXPERTS), jnp.uint32) >> 10) * slow
    expert = jnp.argsort(wait, axis=-1)[..., :TOP].astype(jnp.int32)
    chosen = jax.nn.one_hot(expert, EXPERTS, dtype=jnp.int32)
    in_line = jnp.cumsum(chosen.reshape(*devices, TOKENS * TOP, EXPERTS), axis=2) - 1
    slot = jnp.sum(in_line.reshape(chosen.shape) * chosen, axis=-1)

    def one(key, rows, columns):
        return (jax.random.normal(key, (rows, columns), jnp.float32) * rows**-0.5).astype(jnp.bfloat16)

    def weights(key, rows, columns):
        return jax.lax.map(lambda k: one(k, rows, columns), jax.random.split(key, EXPERTS))

    return {
        "x": jax.random.normal(kx, (*devices, TOKENS, D), jnp.float32).astype(jnp.bfloat16),
        "expert": expert,
        "slot": slot,
        "gate": jax.nn.softmax(jax.random.normal(kg, expert.shape, jnp.float32)),
        "w_gate": weights(k1, D, FF),
        "w_up": weights(k2, D, FF),
        "w_down": weights(k3, FF, D),
        "s_gate": one(k4, D, SHARED_FF),
        "s_up": one(k5, D, SHARED_FF),
        "s_down": one(k6, SHARED_FF, D),
    }


def einsum(form, a, b):
    return jnp.einsum(form, a.astype(jnp.float32), b.astype(jnp.float32))


def for_all(x, s_gate, s_up, s_down):
    h = jax.nn.silu(einsum("...d,df->...f", x, s_gate)) * einsum("...d,df->...f", x, s_up)
    return einsum("...f,fd->...d", h.astype(jnp.bfloat16), s_down)


def reference(x, expert, slot, gate, w_gate, w_up, w_down, s_gate, s_up, s_down):
    to_expert = jax.nn.one_hot(expert, EXPERTS, dtype=jnp.bfloat16)
    to_slot = jax.nn.one_hot(slot, SLOTS, dtype=jnp.bfloat16)
    weighted = to_expert * gate[..., None].astype(jnp.bfloat16)
    dispatch = einsum("abtke,abtkc->abtec", to_expert, to_slot).astype(jnp.bfloat16)
    combine = einsum("abtke,abtkc->abtec", weighted, to_slot).astype(jnp.bfloat16)
    z = einsum("abtec,abtd->aebcd", dispatch, x).astype(jnp.bfloat16)
    h = jax.nn.silu(einsum("aebcd,edf->aebcf", z, w_gate))
    h = (h * einsum("aebcd,edf->aebcf", z, w_up)).astype(jnp.bfloat16)
    out = einsum("aebcf,efd->aebcd", h, w_down).astype(jnp.bfloat16)
    y = einsum("abtec,aebcd->abtd", combine, out)
    return (y + for_all(x, s_gate, s_up, s_down)).astype(jnp.bfloat16)
```

```python
import jax
import jax.numpy as jnp
from jax import lax
from jax.sharding import PartitionSpec as P


def mm(form, a, b):
    return jnp.einsum(form, a, b, preferred_element_type=jnp.float32)


def solution(mesh):
    members = mesh.shape["ep"]

    def body(x, expert, slot, gate, w_gate, w_up, w_down, s_gate, s_up, s_down):
        x, expert, slot, gate = x[0, 0], expert[0, 0], slot[0, 0], gate[0, 0]
        local, depth, width = w_gate.shape
        tokens, top = expert.shape
        slots = 5 * tokens * top // (4 * members * local)
        rows = local * slots
        code = jnp.where(slot < slots, expert * slots + slot, -1)
        xs = lax.all_gather(x, "ep")
        codes = lax.all_gather(code, "ep") - lax.axis_index("ep") * rows
        gates = lax.all_gather(gate.astype(jnp.bfloat16), "ep")
        row = jnp.arange(rows, dtype=jnp.int32)
        hit = codes[..., None] == row
        dispatch = jnp.any(hit, axis=2).astype(jnp.bfloat16)
        combine = jnp.sum(jnp.where(hit, gates[..., None], 0), axis=2, dtype=jnp.bfloat16)
        z = mm("str,std->srd", dispatch, xs).astype(jnp.bfloat16)
        z = z.reshape(members, local, slots, depth).transpose(1, 0, 2, 3).reshape(local, members * slots, depth)
        h = jax.nn.silu(mm("ecd,edf->ecf", z, w_gate)) * mm("ecd,edf->ecf", z, w_up)
        out = mm("ecf,efd->ecd", h.astype(jnp.bfloat16), w_down).astype(jnp.bfloat16)
        out = out.reshape(local, members, slots, depth).transpose(1, 0, 2, 3).reshape(members, rows, depth)
        y = mm("str,srd->std", combine, out).astype(jnp.bfloat16)
        y = lax.psum_scatter(y, "ep", scatter_dimension=0)
        h = jax.nn.silu(mm("td,df->tf", x, s_gate)) * mm("td,df->tf", x, s_up)
        shared = mm("tf,fd->td", h.astype(jnp.bfloat16), s_down)
        return (y.astype(jnp.float32) + shared).astype(jnp.bfloat16)[None, None]

    own = P("dp", "ep", None, None)
    experts, whole = P("ep", None, None), P(None, None)
    return jax.shard_map(
        body,
        mesh=mesh,
        in_specs=(own, own, own, own, experts, experts, experts, whole, whole, whole),
        out_specs=own,
        check_vma=False,
    )
```

```python
import functools

import jax
import jax.numpy as jnp
from jax import lax
from jax.experimental import pallas as pl
from jax.experimental.pallas import tpu as pltpu
from jax.sharding import PartitionSpec as P

F32, BF16 = jnp.float32, jnp.bfloat16
MESH = pl.DeviceIdType.MESH
C = 512
UNITS = 8


def dot(a, b):
    return jnp.dot(a, b, preferred_element_type=F32)


def moe_kernel(
    dims, pk, x, wg, wu, wd, sg, su, sd, y,
    xg, acc, ring, hs, zb, dm, wm, cg,
    ld_sem, cg_send, cg_recv, ag_send, ag_recv, ring_sem, rs_send, rs_recv, out_sem,
):
    members, local, slots, top, chunks, parts = dims
    T = 256
    rows = local * slots
    M = members * slots
    K = chunks
    me = lax.axis_index("ep")
    core, yy, xx = me % 2, (me // 2) % 2, me // 4
    mate, ynbr, xnbr = me + 1 - 2 * core, me + 2 - 4 * yy, me + 4 - 8 * xx
    diag = ynbr + 4 - 8 * xx
    n_shared, n_routed, n_down = 4 * K, 2 * local * K, (local + 2) * K

    def unit_copy(src, r0, c0, down, n):
        slot = n % UNITS
        for j in range(parts):
            if down:
                piece = src.at[pl.ds(r0 + j * C, C), pl.ds(c0, C)]
            else:
                piece = src.at[pl.ds(r0, C), pl.ds(c0 + j * C, C)]
            pltpu.make_async_copy(piece, ring.at[slot, j], ring_sem.at[slot]).start()

    def unit_wait(n):
        slot = n % UNITS
        pltpu.make_async_copy(ring.at[slot], ring.at[slot], ring_sem.at[slot]).wait()
        return slot

    def start_shared(i, q, n):
        unit_copy(sg if q % 2 == 0 else su, pl.multiple_of(i * C, C), (q // 2) * parts * C, False, n)

    def start_routed(k, q, n):
        w = wg if q % 2 == 0 else wu
        unit_copy(w.at[q // 2], pl.multiple_of(k * C, C), 0, False, n)

    def start_down(k, m, n):
        c0 = pl.multiple_of(k * C, C)
        if m < local:
            unit_copy(wd.at[m], 0, c0, True, n)
        else:
            unit_copy(sd, (m - local) * parts * C, c0, True, n)

    def blk(k, s, off=0, n=T):
        return xg.at[k, pl.ds(pl.multiple_of(s * T + off, 128), n)]

    H = T // 2
    routes = (
        (me, 0, T, xnbr), (me, 0, T, ynbr), (me, 0, T, mate),
        (xnbr, 0, H, ynbr), (ynbr, H, H, xnbr),
        (xnbr, 0, T, mate), (ynbr, 0, T, mate), (diag, 0, H, mate), (diag, H, H, mate),
    )
    mx, my, md = mate + 4 - 8 * xx, mate + 2 - 4 * yy, mate + 2 - 4 * yy + 4 - 8 * xx
    landed = (
        (xnbr, 0, T), (ynbr, 0, T), (mate, 0, T), (diag, 0, H), (diag, H, H),
        (mx, 0, T), (my, 0, T), (md, 0, H), (md, H, H),
    )

    def route(kind, k, ref, dev):
        return pltpu.make_async_remote_copy(
            src_ref=ref, dst_ref=ref, send_sem=ag_send.at[kind, k], recv_sem=ag_recv.at[kind, k],
            device_id={"ep": dev}, device_id_type=MESH,
        )

    def ag_start(kinds, k):
        for kind in kinds:
            s, off, n, dev = routes[kind]
            route(kind, k, blk(k, s, off, n), dev).start()

    def ag_sent(kinds, k):
        for kind in kinds:
            s, off, n, dev = routes[kind]
            route(kind, k, blk(k, s, off, n), dev).wait_send()

    def ag_wait(kinds, k):
        for kind in kinds:
            s, off, n = landed[kind]
            route(kind, k, blk(k, s, off, n), mate).wait_recv()

    def comm_a(k):
        ag_wait((0, 1), k)

        @pl.when(k >= 2)
        def _():
            ag_sent(range(9), k - 2)

        ag_start((3, 4, 5, 6), k)

        @pl.when(k + 2 < K)
        def _():
            ag_start((0, 1, 2), k + 2)

    def comm_b(k):
        ag_wait((3, 4), k)
        ag_start((7, 8), k)

    def own_load(k):
        return pltpu.make_async_copy(x.at[:, pl.ds(pl.multiple_of(k * C, C), C)], blk(k, me), ld_sem.at[k])

    for k in range(K):
        own_load(k).start()
    for n in range(UNITS):
        start_shared(n // 4, n % 4, n)
    barrier = pltpu.get_barrier_semaphore()
    for d in range(1, members):
        pl.semaphore_signal(barrier, inc=1, device_id={"ep": (me + d) % members}, device_id_type=MESH)
    pl.semaphore_wait(barrier, members - 1)

    def code_copy(d, src, dst, dev):
        return pltpu.make_async_remote_copy(
            src_ref=src, dst_ref=dst, send_sem=cg_send.at[d], recv_sem=cg_recv.at[d],
            device_id={"ep": dev}, device_id_type=MESH,
        )

    own_load(0).wait()
    ag_start((0, 1, 2), 0)
    for d in range(1, members):
        code_copy(d, pk, cg.at[me], (me + d) % members).start()
    own_load(1).wait()
    ag_start((0, 1, 2), 1)
    cg[me] = pk[...]

    def shared_step(i, _):
        @pl.when(i >= 2)
        def _():
            own_load(i).wait()

        xo = blk(i, me)
        for half in range(2):
            for t in range(2):
                q = 2 * half + t
                n = 4 * i + q
                slot = unit_wait(n)
                for j in range(parts):
                    cols = pl.ds((t * parts + j) * C, C)
                    old = jnp.where(i > 0, acc[3 + half, :T, cols], 0.0)
                    acc[3 + half, :T, cols] = old + dot(xo[...], ring[slot, j])

                @pl.when(i < K - 2)
                def _():
                    start_shared(i + 2, q, n + UNITS)

                for late in range(2):
                    @pl.when(i == K - 2 + late)
                    def _():
                        start_routed(0, 4 * late + q, n + UNITS)

        @pl.when(i == 3)
        def _():
            comm_a(0)

        @pl.when(i == 7)
        def _():
            comm_a(1)
        return 0

    lax.fori_loop(0, K, shared_step, 0)
    for half in range(2):
        for j in range(parts):
            g = acc[3 + half, :T, pl.ds(j * C, C)]
            u = acc[3 + half, :T, pl.ds((parts + j) * C, C)]
            hs[half * parts + j] = (jax.nn.silu(g) * u).astype(BF16)

    zb[pl.ds(local * M, members * T - local * M)] = jnp.zeros((members * T - local * M, C), BF16)
    for d in range(1, members):
        code_copy(d, pk, cg.at[(me + members - d) % members], mate).wait_recv()

    def tables(s, _):
        codes = cg[s]
        row = lax.broadcasted_iota(jnp.int32, (T, T), 0)
        row = jnp.where(row < rows, row + me * rows, -2).astype(F32)
        hit = jnp.zeros((T, T), F32)
        weight = jnp.zeros((T, T), F32)
        for j in range(top):
            same = codes[j:j + 1, :] == row
            hit = jnp.where(same, 1.0, hit)
            weight = jnp.where(same, codes[8 + j:9 + j, :], weight)
        dm[s] = hit.astype(BF16)
        wm[s] = weight.T.astype(BF16)
        return 0

    lax.fori_loop(0, members, tables, 0)
    comm_b(0)

    def routed_step(k, _):
        ag_wait((2, 5, 6, 7, 8), k)
        for s in range(members):
            z = dot(dm[s, :rows], xg[k, pl.ds(s * T, T)]).astype(BF16)
            for e in range(local):
                zb[pl.ds(e * M + s * slots, slots)] = z[e * slots:(e + 1) * slots]

        def expert(e):
            z = zb[pl.ds(e * M, M)]
            for t in range(2):
                q = 2 * e + t
                n = n_shared + 2 * local * k + q
                slot = unit_wait(n)
                for j in range(parts):
                    cols = pl.ds((t * parts + j) * C, C)
                    old = jnp.where(k > 0, acc[e, :, cols], 0.0)
                    acc[e, :, cols] = old + dot(z, ring[slot, j])
                ahead = q + UNITS
                if ahead < 2 * local:
                    start_routed(k, ahead, n + UNITS)
                else:
                    ahead -= 2 * local

                    @pl.when(k + 1 < K)
                    def _():
                        start_routed(k + 1, ahead, n + UNITS)

                    @pl.when(k + 1 == K)
                    def _():
                        start_down(ahead // (local + 2), ahead % (local + 2), n + UNITS)

        for e in range(3):
            expert(e)

        @pl.when(k + 2 < K)
        def _():
            comm_a(k + 2)

        for e in range(3, local):
            expert(e)

        @pl.when(k + 1 < K)
        def _():
            comm_b(k + 1)
        return 0

    lax.fori_loop(0, K, routed_step, 0)
    for k in range(K - 2, K):
        ag_sent(range(9), k)

    for e in range(local):
        for j in range(parts):
            g = acc[e, :, pl.ds(j * C, C)]
            u = acc[e, :, pl.ds((parts + j) * C, C)]
            xg[6 + j, pl.ds(e * M, M)] = (jax.nn.silu(g) * u).astype(BF16)

    spans = ((0, T), (T, T), (2 * T, T), (3 * T, T), (4 * T, H), (4 * T + H, H), (5 * T, T), (6 * T, T))
    targets = (mate, mate, mate, mate, xnbr, ynbr, xnbr, ynbr)
    mine, theirs = (diag, xnbr, ynbr, me), (md, mx, my, mate)

    def rs_copy(kind, k):
        off, n = spans[kind]
        return pltpu.make_async_remote_copy(
            src_ref=xg.at[4 + k % 2, pl.ds(off, n)], dst_ref=xg.at[k % 4, pl.ds(off, n)],
            send_sem=rs_send.at[kind, k % 2], recv_sem=rs_recv.at[kind, k % 4],
            device_id={"ep": targets[kind]}, device_id_type=MESH,
        )

    def rs_free(kinds, k):
        @pl.when(k >= 2)
        def _():
            for kind in kinds:
                rs_copy(kind, k - 2).wait_send()

    def got(kind, k, lo=0, n=None):
        off, size = spans[kind]
        return xg[k % 4, pl.ds(off + lo, size if n is None else n)].astype(F32)

    def part(r, k):
        return acc.at[k % 4, pl.ds(0, T), pl.ds(r * C, C)]

    def compute(k):
        base = n_shared + n_routed + (local + 2) * k

        def refill(m):
            ahead = m + UNITS
            ks, ms = ahead // (local + 2), ahead % (local + 2)

            @pl.when(k + ks < K)
            def _():
                start_down(k + ks, ms, base + m + UNITS)

        for e in range(local):
            slot = unit_wait(base + e)
            out = dot(xg[6, pl.ds(e * M, M)], ring[slot, 0])
            for j in range(1, parts):
                out = out + dot(xg[6 + j, pl.ds(e * M, M)], ring[slot, j])
            out = out.astype(BF16)
            for s in range(members):
                zb[pl.ds(s * T + e * slots, slots)] = out[s * slots:(s + 1) * slots]
            refill(e)
        rs_free(range(4), k)
        for r in range(4):
            s = theirs[r]
            p = dot(wm[s], zb[pl.ds(pl.multiple_of(s * T, T), T)])
            xg[4 + k % 2, pl.ds(r * T, T)] = p.astype(BF16)
            rs_copy(r, k).start()
        for r in range(4):
            s = mine[r]
            part(r, k)[...] = dot(wm[s], zb[pl.ds(pl.multiple_of(s * T, T), T)])
        rs_copy(0, k).wait_recv()
        rs_free((4, 5), k)
        xg[4 + k % 2, pl.ds(4 * T, T)] = (part(0, k)[...] + got(0, k)).astype(BF16)
        rs_copy(4, k).start()
        rs_copy(5, k).start()
        total = None
        for half in range(2):
            slot = unit_wait(base + local + half)
            for j in range(parts):
                term = dot(hs[half * parts + j], ring[slot, j])
                total = term if total is None else total + term
            if half == 1:
                part(4, k)[...] = total
            refill(local + half)

    def pass_on(k):
        for kind in (1, 2, 4, 5):
            rs_copy(kind, k).wait_recv()
        rs_free((6, 7), k)
        out = xg.at[4 + k % 2]
        px, py = part(1, k), part(2, k)
        out[pl.ds(5 * T, H)] = (px[:H] + got(1, k, 0, H)).astype(BF16)
        out[pl.ds(5 * T + H, H)] = (px[H:] + got(1, k, H, H) + got(5, k)).astype(BF16)
        rs_copy(6, k).start()
        out[pl.ds(6 * T, H)] = (py[:H] + got(2, k, 0, H) + got(4, k)).astype(BF16)
        out[pl.ds(6 * T + H, H)] = (py[H:] + got(2, k, H, H)).astype(BF16)
        rs_copy(7, k).start()

    def out_copy(k):
        return pltpu.make_async_copy(
            xg.at[9, pl.ds((k % 2) * T, T)], y.at[:, pl.ds(pl.multiple_of(k * C, C), C)], out_sem.at[k % 2]
        )

    def finish(k):
        for kind in (3, 6, 7):
            rs_copy(kind, k).wait_recv()

        @pl.when(k >= 2)
        def _():
            out_copy(k - 2).wait()

        total = part(3, k)[...] + got(3, k) + got(6, k) + got(7, k) + part(4, k)[...]
        xg[9, pl.ds((k % 2) * T, T)] = total.astype(BF16)
        out_copy(k).start()

    def down_step(i, _):
        @pl.when(i < K)
        def _():
            compute(i)

        @pl.when((i >= 1) & (i <= K))
        def _():
            pass_on(i - 1)

        @pl.when(i >= 2)
        def _():
            finish(i - 2)
        return 0

    lax.fori_loop(0, K + 2, down_step, 0)
    for k in range(K - 2, K):
        out_copy(k).wait()
        for kind in range(8):
            rs_copy(kind, k).wait_send()
    for d in range(1, members):
        code_copy(d, pk, cg.at[me], mate).wait_send()


def solution(mesh):
    members = mesh.shape["ep"]

    def body(x, expert, slot, gate, w_gate, w_up, w_down, s_gate, s_up, s_down):
        x, expert, slot, gate = x[0, 0], expert[0, 0], slot[0, 0], gate[0, 0]
        local, depth, width = w_gate.shape
        tokens, top = expert.shape
        slots = 5 * tokens * top // (4 * members * local)
        code = jnp.where(slot < slots, expert * slots + slot, -1).astype(F32)
        weight = gate.astype(BF16).astype(F32)
        pad = jnp.zeros((8 - top, tokens), F32)
        pk = jnp.concatenate([code.T, pad, weight.T, pad])
        chunks, parts = depth // C, width // C
        dims = (members, local, slots, top, chunks, parts)
        rows, M = local * slots, members * slots
        anywhere = pl.BlockSpec(memory_space=pl.ANY)
        dma = pltpu.SemaphoreType.DMA
        out = pl.pallas_call(
            functools.partial(moe_kernel, dims),
            out_shape=jax.ShapeDtypeStruct((tokens, depth), BF16),
            in_specs=[pl.BlockSpec(memory_space=pltpu.VMEM)] + [anywhere] * 7,
            out_specs=anywhere,
            scratch_shapes=[
                pltpu.VMEM((chunks, members * tokens, C), BF16),
                pltpu.VMEM((local, M, 2 * width), F32),
                pltpu.VMEM((UNITS, parts, C, C), BF16),
                pltpu.VMEM((2 * parts, tokens, C), BF16),
                pltpu.VMEM((members * tokens, C), BF16),
                pltpu.VMEM((members, tokens, tokens), BF16),
                pltpu.VMEM((members, tokens, tokens), BF16),
                pltpu.VMEM((members, 16, tokens), F32),
                dma((chunks,)), dma((members,)), dma((members,)),
                dma((9, chunks)), dma((9, chunks)), dma((UNITS,)),
                dma((8, 2)), dma((8, 4)), dma((2,)),
            ],
            compiler_params=pltpu.CompilerParams(
                collective_id=0, has_side_effects=True, vmem_limit_bytes=67_000_000
            ),
            name="moe",
        )(pk, x, w_gate, w_up, w_down, s_gate, s_up, s_down)
        return out[None, None]

    own = P("dp", "ep", None, None)
    experts, whole = P("ep", None, None), P(None, None)
    return jax.shard_map(
        body,
        mesh=mesh,
        in_specs=(own, own, own, own, experts, experts, experts, whole, whole, whole),
        out_specs=own,
        check_vma=False,
    )
```

```python
import functools

import jax
import jax.numpy as jnp
from jax import lax
from jax.experimental import pallas as pl
from jax.experimental.pallas import tpu as pltpu
from jax.sharding import PartitionSpec as P

F32, BF16 = jnp.float32, jnp.bfloat16
MESH = pl.DeviceIdType.MESH
C = 512
UNITS = 8


def dot(a, b):
    return jnp.dot(a, b, preferred_element_type=F32)


def moe_kernel(
    dims, expert, slot_of, gate, x, wg, wu, wd, sg, su, sd, y,
    xg, acc, ring, hs, zb, dm, wm, cg, pk,
    ld_sem, cg_send, cg_recv, ag_send, ag_recv, ring_sem, rs_send, rs_recv, out_sem,
):
    members, local, slots, top, chunks, parts = dims
    T = 256
    rows = local * slots
    M = members * slots
    K = chunks
    me = lax.axis_index("ep")
    core, yy, xx = me % 2, (me // 2) % 2, me // 4
    mate, ynbr, xnbr = me + 1 - 2 * core, me + 2 - 4 * yy, me + 4 - 8 * xx
    diag = ynbr + 4 - 8 * xx
    n_shared, n_routed, n_down = 4 * K, 2 * local * K, (local + 2) * K

    def unit_copy(src, r0, c0, down, n):
        slot = n % UNITS
        for j in range(parts):
            if down:
                piece = src.at[pl.ds(r0 + j * C, C), pl.ds(c0, C)]
            else:
                piece = src.at[pl.ds(r0, C), pl.ds(c0 + j * C, C)]
            pltpu.make_async_copy(piece, ring.at[slot, j], ring_sem.at[slot]).start()

    def unit_wait(n):
        slot = n % UNITS
        pltpu.make_async_copy(ring.at[slot], ring.at[slot], ring_sem.at[slot]).wait()
        return slot

    def start_shared(i, q, n):
        unit_copy(sg if q % 2 == 0 else su, pl.multiple_of(i * C, C), (q // 2) * parts * C, False, n)

    def start_routed(k, q, n):
        w = wg if q % 2 == 0 else wu
        unit_copy(w.at[q // 2], pl.multiple_of(k * C, C), 0, False, n)

    def start_down(k, m, n):
        c0 = pl.multiple_of(k * C, C)
        if m < local:
            unit_copy(wd.at[m], 0, c0, True, n)
        else:
            unit_copy(sd, (m - local) * parts * C, c0, True, n)

    def blk(k, s, off=0, n=T):
        return xg.at[k, pl.ds(pl.multiple_of(s * T + off, 128), n)]

    H = T // 2
    routes = (
        (me, 0, T, xnbr), (me, 0, T, ynbr), (me, 0, T, mate),
        (xnbr, 0, H, ynbr), (ynbr, H, H, xnbr),
        (xnbr, 0, T, mate), (ynbr, 0, T, mate), (diag, 0, H, mate), (diag, H, H, mate),
    )
    mx, my, md = mate + 4 - 8 * xx, mate + 2 - 4 * yy, mate + 2 - 4 * yy + 4 - 8 * xx
    landed = (
        (xnbr, 0, T), (ynbr, 0, T), (mate, 0, T), (diag, 0, H), (diag, H, H),
        (mx, 0, T), (my, 0, T), (md, 0, H), (md, H, H),
    )

    def route(kind, k, ref, dev):
        return pltpu.make_async_remote_copy(
            src_ref=ref, dst_ref=ref, send_sem=ag_send.at[kind, k], recv_sem=ag_recv.at[kind, k],
            device_id={"ep": dev}, device_id_type=MESH,
        )

    def ag_start(kinds, k):
        for kind in kinds:
            s, off, n, dev = routes[kind]
            route(kind, k, blk(k, s, off, n), dev).start()

    def ag_sent(kinds, k):
        for kind in kinds:
            s, off, n, dev = routes[kind]
            route(kind, k, blk(k, s, off, n), dev).wait_send()

    def ag_wait(kinds, k):
        for kind in kinds:
            s, off, n = landed[kind]
            route(kind, k, blk(k, s, off, n), mate).wait_recv()

    def comm_a(k):
        ag_wait((0, 1), k)

        @pl.when(k >= 2)
        def _():
            ag_sent(range(9), k - 2)

        ag_start((3, 4, 5, 6), k)

        @pl.when(k + 2 < K)
        def _():
            ag_start((0, 1, 2), k + 2)

    def comm_b(k):
        ag_wait((3, 4), k)
        ag_start((7, 8), k)

    def own_load(k):
        return pltpu.make_async_copy(x.at[:, pl.ds(pl.multiple_of(k * C, C), C)], blk(k, me), ld_sem.at[k])

    for k in range(K):
        own_load(k).start()
    for n in range(UNITS):
        start_shared(n // 4, n % 4, n)
    pk[...] = jnp.zeros(pk.shape, F32)
    for j in range(top):
        place = slot_of[j]
        pk[j:j + 1] = jnp.where(place < slots, expert[j] * slots + place, -1).astype(F32)
        pk[8 + j:9 + j] = gate[j].astype(BF16).astype(F32)
    barrier = pltpu.get_barrier_semaphore()
    for d in range(1, members):
        pl.semaphore_signal(barrier, inc=1, device_id={"ep": (me + d) % members}, device_id_type=MESH)
    pl.semaphore_wait(barrier, members - 1)

    def code_copy(d, src, dst, dev):
        return pltpu.make_async_remote_copy(
            src_ref=src, dst_ref=dst, send_sem=cg_send.at[d], recv_sem=cg_recv.at[d],
            device_id={"ep": dev}, device_id_type=MESH,
        )

    own_load(0).wait()
    ag_start((0, 1, 2), 0)
    for d in range(1, members):
        code_copy(d, pk, cg.at[me], (me + d) % members).start()
    own_load(1).wait()
    ag_start((0, 1, 2), 1)
    cg[me] = pk[...]

    for k in range(2, K):
        own_load(k).wait()

    def shared_step(i, _):
        xo = blk(i, me)
        held = [unit_wait(4 * i + q) for q in range(4)]
        for half in range(2):
            for t in range(2):
                for j in range(parts):
                    cols = pl.ds((t * parts + j) * C, C)
                    old = jnp.where(i > 0, acc[3 + half, :T, cols], 0.0)
                    acc[3 + half, :T, cols] = old + dot(xo[...], ring[held[2 * half + t], j])

        @pl.when(i < K - 2)
        def _():
            for q in range(4):
                start_shared(i + 2, q, 4 * i + q + UNITS)

        for late in range(2):
            @pl.when(i == K - 2 + late)
            def _():
                for q in range(4):
                    start_routed(0, 4 * late + q, 4 * i + q + UNITS)

        @pl.when(i == 3)
        def _():
            comm_a(0)

        @pl.when(i == 7)
        def _():
            comm_a(1)
        return 0

    lax.fori_loop(0, K, shared_step, 0)
    for half in range(2):
        for j in range(parts):
            g = acc[3 + half, :T, pl.ds(j * C, C)]
            u = acc[3 + half, :T, pl.ds((parts + j) * C, C)]
            hs[half * parts + j] = (jax.nn.silu(g) * u).astype(BF16)

    zb[pl.ds(local * M, members * T - local * M)] = jnp.zeros((members * T - local * M, C), BF16)
    for d in range(1, members):
        code_copy(d, pk, cg.at[(me + members - d) % members], mate).wait_recv()

    def tables(s, _):
        codes = cg[s]
        row = lax.broadcasted_iota(jnp.int32, (T, T), 0)
        row = jnp.where(row < rows, row + me * rows, -2).astype(F32)
        hit = jnp.zeros((T, T), F32)
        weight = jnp.zeros((T, T), F32)
        for j in range(top):
            same = codes[j:j + 1, :] == row
            hit = jnp.where(same, 1.0, hit)
            weight = jnp.where(same, codes[8 + j:9 + j, :], weight)
        dm[s] = hit.astype(BF16)
        wm[s] = weight.T.astype(BF16)
        return 0

    lax.fori_loop(0, members, tables, 0)
    comm_b(0)

    def hidden(e):
        for j in range(parts):
            g = acc[e, :, pl.ds(j * C, C)]
            u = acc[e, :, pl.ds((parts + j) * C, C)]
            xg[6 + j, pl.ds(e * M, M)] = (jax.nn.silu(g) * u).astype(BF16)

    groups = [list(range(e, min(e + 2, local))) for e in range(0, local, 2)]

    def routed_step(k, last):
        base = n_shared + 2 * local * k
        ag_wait((2, 5, 6, 7, 8), k)
        for group in groups:
            units = [2 * e + t for e in group for t in range(2)]
            held = [unit_wait(base + q) for q in units]
            if group[0] == 0:
                for s in range(members):
                    z = dot(dm[s, :rows], xg[k, pl.ds(s * T, T)]).astype(BF16)
                    for e in range(local):
                        zb[pl.ds(e * M + s * slots, slots)] = z[e * slots:(e + 1) * slots]
            elif last:
                hidden(group[0] - 1)
            for e in group:
                z = zb[pl.ds(e * M, M)]
                for t in range(2):
                    for j in range(parts):
                        cols = pl.ds((t * parts + j) * C, C)
                        old = acc[e, :, cols]
                        if not last:
                            old = jnp.where(k > 0, old, 0.0)
                        acc[e, :, cols] = old + dot(z, ring[held[units.index(2 * e + t)], j])
                if last and e != group[-1]:
                    hidden(e)
            for q in units:
                ahead = q + UNITS
                if ahead < 2 * local:
                    start_routed(k, ahead, base + q + UNITS)
                elif not last:
                    start_routed(k + 1, ahead - 2 * local, base + q + UNITS)
                else:
                    ahead -= 2 * local
                    start_down(ahead // (local + 2), ahead % (local + 2), base + q + UNITS)
            if group is groups[1] and not last:
                @pl.when(k + 2 < K)
                def _():
                    comm_a(k + 2)
        if not last:
            comm_b(k + 1)
        return 0

    lax.fori_loop(0, K - 1, lambda k, _: routed_step(k, False), 0)
    ag_sent(range(9), K - 2)
    routed_step(K - 1, True)
    hidden(groups[-1][-1])
    ag_sent(range(9), K - 1)

    spans = ((0, T), (T, T), (2 * T, T), (3 * T, T), (4 * T, H), (4 * T + H, H), (5 * T, T), (6 * T, T))
    targets = (mate, mate, mate, mate, xnbr, ynbr, xnbr, ynbr)
    mine, theirs = (diag, xnbr, ynbr, me), (md, mx, my, mate)

    def rs_copy(kind, k):
        off, n = spans[kind]
        return pltpu.make_async_remote_copy(
            src_ref=xg.at[4 + k % 2, pl.ds(off, n)], dst_ref=xg.at[k % 4, pl.ds(off, n)],
            send_sem=rs_send.at[kind, k % 2], recv_sem=rs_recv.at[kind, k % 4],
            device_id={"ep": targets[kind]}, device_id_type=MESH,
        )

    def rs_free(kinds, k):
        @pl.when(k >= 2)
        def _():
            for kind in kinds:
                rs_copy(kind, k - 2).wait_send()

    def got(kind, k, lo=0, n=None):
        off, size = spans[kind]
        return xg[k % 4, pl.ds(off + lo, size if n is None else n)].astype(F32)

    def part(r, k):
        return acc.at[k % 4, pl.ds(0, T), pl.ds(r * C, C)]

    def compute(k):
        base = n_shared + n_routed + (local + 2) * k

        def refill(ms):
            @pl.when(k + 1 < K)
            def _():
                for m in ms:
                    ahead = m + UNITS
                    if ahead < 2 * (local + 2):
                        start_down(k + 1, ahead - (local + 2), base + ahead)

            if ms[-1] + UNITS >= 2 * (local + 2):
                @pl.when(k + 2 < K)
                def _():
                    start_down(k + 2, ms[-1] + UNITS - 2 * (local + 2), base + ms[-1] + UNITS)

        for group in (range(3), range(3, local)):
            held = [unit_wait(base + e) for e in group]
            for slot, e in zip(held, group):
                out = dot(xg[6, pl.ds(e * M, M)], ring[slot, 0])
                for j in range(1, parts):
                    out = out + dot(xg[6 + j, pl.ds(e * M, M)], ring[slot, j])
                out = out.astype(BF16)
                for s in range(members):
                    zb[pl.ds(s * T + e * slots, slots)] = out[s * slots:(s + 1) * slots]
            refill(group)
        rs_free(range(4), k)
        for r in range(4):
            s = theirs[r]
            p = dot(wm[s], zb[pl.ds(pl.multiple_of(s * T, T), T)])
            xg[4 + k % 2, pl.ds(r * T, T)] = p.astype(BF16)
            rs_copy(r, k).start()
        for r in range(4):
            s = mine[r]
            part(r, k)[...] = dot(wm[s], zb[pl.ds(pl.multiple_of(s * T, T), T)])
        rs_copy(0, k).wait_recv()
        rs_free((4, 5), k)
        xg[4 + k % 2, pl.ds(4 * T, T)] = (part(0, k)[...] + got(0, k)).astype(BF16)
        rs_copy(4, k).start()
        rs_copy(5, k).start()
        held = [unit_wait(base + local + half) for half in range(2)]
        total = None
        for half in range(2):
            for j in range(parts):
                term = dot(hs[half * parts + j], ring[held[half], j])
                total = term if total is None else total + term
        part(4, k)[...] = total
        refill((local, local + 1))

    def pass_on(k):
        for kind in (1, 2, 4, 5):
            rs_copy(kind, k).wait_recv()
        rs_free((6, 7), k)
        out = xg.at[4 + k % 2]
        px, py = part(1, k), part(2, k)
        out[pl.ds(5 * T, H)] = (px[:H] + got(1, k, 0, H)).astype(BF16)
        out[pl.ds(5 * T + H, H)] = (px[H:] + got(1, k, H, H) + got(5, k)).astype(BF16)
        rs_copy(6, k).start()
        out[pl.ds(6 * T, H)] = (py[:H] + got(2, k, 0, H) + got(4, k)).astype(BF16)
        out[pl.ds(6 * T + H, H)] = (py[H:] + got(2, k, H, H)).astype(BF16)
        rs_copy(7, k).start()

    def out_copy(k):
        return pltpu.make_async_copy(
            xg.at[9, pl.ds((k % 2) * T, T)], y.at[:, pl.ds(pl.multiple_of(k * C, C), C)], out_sem.at[k % 2]
        )

    def finish(k):
        for kind in (3, 6, 7):
            rs_copy(kind, k).wait_recv()

        @pl.when(k >= 2)
        def _():
            out_copy(k - 2).wait()

        total = part(3, k)[...] + got(3, k) + got(6, k) + got(7, k) + part(4, k)[...]
        xg[9, pl.ds((k % 2) * T, T)] = total.astype(BF16)
        out_copy(k).start()

    def down_step(i, _):
        @pl.when(i < K)
        def _():
            compute(i)

        @pl.when((i >= 1) & (i <= K))
        def _():
            pass_on(i - 1)

        @pl.when(i >= 2)
        def _():
            finish(i - 2)
        return 0

    lax.fori_loop(0, K + 2, down_step, 0)
    for k in range(K - 2, K):
        out_copy(k).wait()
        for kind in range(8):
            rs_copy(kind, k).wait_send()
    for d in range(1, members):
        code_copy(d, pk, cg.at[me], mate).wait_send()


def solution(mesh):
    members = mesh.shape["ep"]

    def body(x, expert, slot, gate, w_gate, w_up, w_down, s_gate, s_up, s_down):
        local, depth, width = w_gate.shape
        tokens, top = expert.shape[2:]
        x, (expert, slot, gate) = x[0, 0], (jnp.transpose(v[0], (2, 0, 1)) for v in (expert, slot, gate))
        slots = 5 * tokens * top // (4 * members * local)
        chunks, parts = depth // C, width // C
        dims = (members, local, slots, top, chunks, parts)
        rows, M = local * slots, members * slots
        anywhere = pl.BlockSpec(memory_space=pl.ANY)
        dma = pltpu.SemaphoreType.DMA
        out = pl.pallas_call(
            functools.partial(moe_kernel, dims),
            out_shape=jax.ShapeDtypeStruct((tokens, depth), BF16),
            in_specs=[pl.BlockSpec(memory_space=pltpu.VMEM)] * 3 + [anywhere] * 7,
            out_specs=anywhere,
            scratch_shapes=[
                pltpu.VMEM((chunks, members * tokens, C), BF16),
                pltpu.VMEM((local, M, 2 * width), F32),
                pltpu.VMEM((UNITS, parts, C, C), BF16),
                pltpu.VMEM((2 * parts, tokens, C), BF16),
                pltpu.VMEM((members * tokens, C), BF16),
                pltpu.VMEM((members, tokens, tokens), BF16),
                pltpu.VMEM((members, tokens, tokens), BF16),
                pltpu.VMEM((members, 16, tokens), F32),
                pltpu.VMEM((16, tokens), F32),
                dma((chunks,)), dma((members,)), dma((members,)),
                dma((9, chunks)), dma((9, chunks)), dma((UNITS,)),
                dma((8, 2)), dma((8, 4)), dma((2,)),
            ],
            compiler_params=pltpu.CompilerParams(
                collective_id=0, has_side_effects=True, vmem_limit_bytes=67_000_000
            ),
            name="moe",
        )(expert, slot, gate, x, w_gate, w_up, w_down, s_gate, s_up, s_down)
        return out[None, None]

    own = P("dp", "ep", None, None)
    experts, whole = P("ep", None, None), P(None, None)
    return jax.shard_map(
        body,
        mesh=mesh,
        in_specs=(own, own, own, own, experts, experts, experts, whole, whole, whole),
        out_specs=own,
        check_vma=False,
    )
```

```python
import functools

import jax
import jax.numpy as jnp
from jax import lax
from jax.experimental import pallas as pl
from jax.experimental.pallas import tpu as pltpu
from jax.sharding import PartitionSpec as P

F32, BF16 = jnp.float32, jnp.bfloat16
MESH = pl.DeviceIdType.MESH
C = 512
UNITS = 8


def dot(a, b):
    return jnp.dot(a, b, preferred_element_type=F32)


def moe_kernel(
    dims, expert, slot_of, gate, x, wg, wu, wd, sg, su, sd, y,
    xg, acc, ring, hs, zb, dm, wm, cg, pk,
    ld_sem, cg_send, cg_recv, ag_send, ag_recv, ring_sem, rs_send, rs_recv, out_sem,
):
    members, local, slots, top, chunks, parts = dims
    T = 256
    rows = local * slots
    M = members * slots
    K = chunks
    me = lax.axis_index("ep")
    core, yy, xx = me % 2, (me // 2) % 2, me // 4
    mate, ynbr, xnbr = me + 1 - 2 * core, me + 2 - 4 * yy, me + 4 - 8 * xx
    diag = ynbr + 4 - 8 * xx
    n_shared, n_routed, per_down = 2 * K, 2 * local * K, local + 1
    half = pl.multiple_of(core * parts * C, C)

    def unit_copy(src, r0, c0, down, n):
        slot = n % UNITS
        for j in range(parts):
            if down:
                piece = src.at[pl.ds(r0 + j * C, C), pl.ds(c0, C)]
            else:
                piece = src.at[pl.ds(r0, C), pl.ds(c0 + j * C, C)]
            pltpu.make_async_copy(piece, ring.at[slot, j], ring_sem.at[slot]).start(priority=1)

    def unit_wait(n):
        slot = n % UNITS
        pltpu.make_async_copy(ring.at[slot], ring.at[slot], ring_sem.at[slot]).wait()
        return slot

    def start_shared(i, t, n):
        unit_copy((sg, su)[t], pl.multiple_of(i * C, C), half, False, n)

    def start_routed(k, q, n):
        w = wg if q % 2 == 0 else wu
        unit_copy(w.at[q // 2], pl.multiple_of(k * C, C), 0, False, n)

    def start_down(k, m, n):
        c0 = pl.multiple_of(k * C, C)
        if m < local:
            unit_copy(wd.at[m], 0, c0, True, n)
        else:
            unit_copy(sd, half, c0, True, n)

    def blk(k, s, off=0, n=T):
        return xg.at[k, pl.ds(pl.multiple_of(s * T + off, 128), n)]

    H = T // 2
    routes = (
        (me, 0, T, xnbr), (me, 0, T, ynbr), (me, 0, T, mate),
        (xnbr, 0, H, ynbr), (ynbr, H, H, xnbr),
        (xnbr, 0, T, mate), (ynbr, 0, T, mate), (diag, 0, H, mate), (diag, H, H, mate),
    )
    mx, my, md = mate + 4 - 8 * xx, mate + 2 - 4 * yy, mate + 2 - 4 * yy + 4 - 8 * xx
    landed = (
        (xnbr, 0, T), (ynbr, 0, T), (mate, 0, T), (diag, 0, H), (diag, H, H),
        (mx, 0, T), (my, 0, T), (md, 0, H), (md, H, H),
    )

    def route(kind, k, ref, dev):
        return pltpu.make_async_remote_copy(
            src_ref=ref, dst_ref=ref, send_sem=ag_send.at[kind, k], recv_sem=ag_recv.at[kind, k],
            device_id={"ep": dev}, device_id_type=MESH,
        )

    def ag_start(kinds, k):
        for kind in kinds:
            s, off, n, dev = routes[kind]
            route(kind, k, blk(k, s, off, n), dev).start()

    def ag_sent(kinds, k):
        for kind in kinds:
            s, off, n, dev = routes[kind]
            route(kind, k, blk(k, s, off, n), dev).wait_send()

    def ag_wait(kinds, k):
        for kind in kinds:
            s, off, n = landed[kind]
            route(kind, k, blk(k, s, off, n), mate).wait_recv()

    def comm_a(k):
        ag_wait((0, 1), k)

        @pl.when(k >= 2)
        def _():
            ag_sent(range(9), k - 2)

        ag_start((3, 4, 5, 6), k)

        @pl.when(k + 2 < K)
        def _():
            ag_start((0, 1), k + 2)

    def comm_b(k):
        ag_wait((3, 4), k)
        ag_start((7, 8), k)

    def own_load(k):
        return pltpu.make_async_copy(x.at[:, pl.ds(pl.multiple_of(k * C, C), C)], blk(k, me), ld_sem.at[k])

    for k in range(K):
        own_load(k).start()
    for n in range(UNITS):
        start_shared(n // 2, n % 2, n)
    pk[...] = jnp.zeros(pk.shape, F32)
    for j in range(top):
        place = slot_of[j]
        pk[j:j + 1] = jnp.where(place < slots, expert[j] * slots + place, -1).astype(F32)
        pk[8 + j:9 + j] = gate[j].astype(BF16).astype(F32)
    barrier = pltpu.get_barrier_semaphore()
    for d in range(1, members):
        pl.semaphore_signal(barrier, inc=1, device_id={"ep": (me + d) % members}, device_id_type=MESH)
    pl.semaphore_wait(barrier, members - 1)

    def code_copy(d, src, dst, dev):
        return pltpu.make_async_remote_copy(
            src_ref=src, dst_ref=dst, send_sem=cg_send.at[d], recv_sem=cg_recv.at[d],
            device_id={"ep": dev}, device_id_type=MESH,
        )

    own_load(0).wait()
    ag_start((0, 1, 2), 0)
    for d in range(1, members):
        code_copy(d, pk, cg.at[me], (me + d) % members).start()
    own_load(1).wait()
    ag_start((0, 1, 2), 1)
    cg[me] = pk[...]

    for k in range(2, K):
        own_load(k).wait()
        ag_start((2,), k)
    zb[pl.ds(local * M, members * T - local * M)] = jnp.zeros((members * T - local * M, C), BF16)

    def tables(s):
        codes = cg[s]
        row = lax.broadcasted_iota(jnp.int32, (T, T), 0)
        row = jnp.where(row < rows, row + me * rows, -2).astype(F32)
        hit = jnp.zeros((T, T), F32)
        weight = jnp.zeros((T, T), F32)
        for j in range(top):
            same = codes[j:j + 1, :] == row
            hit = jnp.where(same, 1.0, hit)
            weight = jnp.where(same, codes[8 + j:9 + j, :], weight)
        dm[s] = hit.astype(BF16)
        wm[s] = weight.T.astype(BF16)

    def shared_step(i, _):
        ag_wait((2,), i)
        held = [unit_wait(2 * i + t) for t in range(2)]
        both = xg[i, pl.ds(pl.multiple_of((me - core) * T, 2 * T), 2 * T)]
        for t in range(2):
            for j in range(parts):
                cols = pl.ds((t * parts + j) * C, C)
                term = dot(both, ring[held[t], j])
                acc[3, :T, cols] = jnp.where(i > 0, acc[3, :T, cols], 0.0) + term[:T]
                acc[4, :T, cols] = jnp.where(i > 0, acc[4, :T, cols], 0.0) + term[T:]

        @pl.when(i < K - 4)
        def _():
            for t in range(2):
                start_shared(i + 4, t, 2 * i + t + UNITS)

        for late in range(4):
            @pl.when(i == K - 4 + late)
            def _():
                for t in range(2):
                    start_routed(0, 2 * late + t, 2 * i + t + UNITS)

        @pl.when(i == 1)
        def _():
            for d in range(1, members):
                code_copy(d, pk, cg.at[(me + members - d) % members], mate).wait_recv()

        @pl.when(i >= 2)
        def _():
            tables(i - 2)

        @pl.when(i == 4)
        def _():
            comm_a(0)

        @pl.when(i == 8)
        def _():
            comm_a(1)
        return 0

    lax.fori_loop(0, K, shared_step, 0)
    for side in range(2):
        for j in range(parts):
            g = acc[3 + side, :T, pl.ds(j * C, C)]
            u = acc[3 + side, :T, pl.ds((parts + j) * C, C)]
            hs[j, pl.ds(side * T, T)] = (jax.nn.silu(g) * u).astype(BF16)
    comm_b(0)

    def hidden(e):
        for j in range(parts):
            g = acc[e, :, pl.ds(j * C, C)]
            u = acc[e, :, pl.ds((parts + j) * C, C)]
            xg[6 + j, pl.ds(e * M, M)] = (jax.nn.silu(g) * u).astype(BF16)

    groups = [[0], list(range(1, local - 2)), [local - 2], [local - 1]]

    def routed_step(k, last):
        base = n_shared + 2 * local * k
        ag_wait((5, 6, 7, 8), k)
        for group in groups:
            units = [2 * e + t for e in group for t in range(2)]
            held = [unit_wait(base + q) for q in units]
            if group[0] == 0:
                for s in range(members):
                    z = dot(dm[s, :rows], xg[k, pl.ds(s * T, T)]).astype(BF16)
                    for e in range(local):
                        zb[pl.ds(e * M + s * slots, slots)] = z[e * slots:(e + 1) * slots]
            elif last:
                hidden(group[0] - 1)
            for e in group:
                z = zb[pl.ds(e * M, M)]
                for t in range(2):
                    for j in range(parts):
                        cols = pl.ds((t * parts + j) * C, C)
                        old = acc[e, :, cols]
                        if not last:
                            old = jnp.where(k > 0, old, 0.0)
                        acc[e, :, cols] = old + dot(z, ring[held[units.index(2 * e + t)], j])
                if last and e != group[-1]:
                    hidden(e)
            for q in units:
                ahead = q + UNITS
                if ahead < 2 * local:
                    start_routed(k, ahead, base + q + UNITS)
                elif not last:
                    start_routed(k + 1, ahead - 2 * local, base + q + UNITS)
                else:
                    ahead -= 2 * local
                    start_down(ahead // per_down, ahead % per_down, base + q + UNITS)
            if group is groups[1] and not last:
                @pl.when(k + 2 < K)
                def _():
                    comm_a(k + 2)
            if group is groups[2] and not last:
                comm_b(k + 1)
        return 0

    lax.fori_loop(0, K - 1, lambda k, _: routed_step(k, False), 0)
    ag_sent(range(9), K - 2)
    routed_step(K - 1, True)
    hidden(groups[-1][-1])
    ag_sent(range(9), K - 1)

    spans = ((0, T), (T, T), (2 * T, T), (3 * T, T), (4 * T, H), (4 * T + H, H), (5 * T, T), (6 * T, T))
    targets = (mate, mate, mate, mate, xnbr, ynbr, xnbr, ynbr)
    mine, theirs = (diag, xnbr, ynbr, me), (md, mx, my, mate)

    def rs_copy(kind, k):
        off, n = spans[kind]
        return pltpu.make_async_remote_copy(
            src_ref=xg.at[4 + k % 2, pl.ds(off, n)], dst_ref=xg.at[k % 4, pl.ds(off, n)],
            send_sem=rs_send.at[kind, k % 2], recv_sem=rs_recv.at[kind, k % 4],
            device_id={"ep": targets[kind]}, device_id_type=MESH,
        )

    def rs_free(kinds, k):
        @pl.when(k >= 2)
        def _():
            for kind in kinds:
                rs_copy(kind, k - 2).wait_send()

    def got(kind, k, lo=0, n=None):
        off, size = spans[kind]
        return xg[k % 4, pl.ds(off + lo, size if n is None else n)].astype(F32)

    def part(r, k):
        return acc.at[k % 4, pl.ds(0, T), pl.ds(r * C, C)]

    def compute(k):
        base = n_shared + n_routed + per_down * k

        def refill(ms):
            for ks in (1, 2):
                some = [m for m in ms if (m + UNITS) // per_down == ks]
                if some:
                    @pl.when(k + ks < K)
                    def _():
                        for m in some:
                            start_down(k + ks, (m + UNITS) % per_down, base + m + UNITS)

        for group in (range(3), range(3, per_down)):
            held = [unit_wait(base + m) for m in group]
            for slot, e in zip(held, group):
                if e == local:
                    continue
                out = dot(xg[6, pl.ds(e * M, M)], ring[slot, 0])
                for j in range(1, parts):
                    out = out + dot(xg[6 + j, pl.ds(e * M, M)], ring[slot, j])
                out = out.astype(BF16)
                for s in range(members):
                    zb[pl.ds(s * T + e * slots, slots)] = out[s * slots:(s + 1) * slots]
            refill([m for m in group if m < local])
        shared = held[-1]

        def combined(s):
            return dot(wm[s], zb[pl.ds(pl.multiple_of(s * T, T), T)])

        def shared_part(side):
            total = None
            for j in range(parts):
                term = dot(hs[j, pl.ds(pl.multiple_of(side * T, T), T)], ring[shared, j])
                total = term if total is None else total + term
            return total

        def send(r, p):
            xg[4 + k % 2, pl.ds(r * T, T)] = p.astype(BF16)
            rs_copy(r, k).start()

        rs_free(range(4), k)
        for r in range(3):
            send(r, combined(theirs[r]))
        for r in range(3):
            part(r, k)[...] = combined(mine[r])
        rs_copy(0, k).wait_recv()
        rs_free((4, 5), k)
        xg[4 + k % 2, pl.ds(4 * T, T)] = (part(0, k)[...] + got(0, k)).astype(BF16)
        rs_copy(4, k).start()
        rs_copy(5, k).start()
        send(3, combined(theirs[3]) + shared_part(1 - core))
        part(3, k)[...] = combined(mine[3]) + shared_part(core)
        refill([local])

    def pass_on(k):
        for kind in (1, 2, 4, 5):
            rs_copy(kind, k).wait_recv()
        rs_free((6, 7), k)
        out = xg.at[4 + k % 2]
        px, py = part(1, k), part(2, k)
        out[pl.ds(5 * T, H)] = (px[:H] + got(1, k, 0, H)).astype(BF16)
        out[pl.ds(5 * T + H, H)] = (px[H:] + got(1, k, H, H) + got(5, k)).astype(BF16)
        rs_copy(6, k).start()
        out[pl.ds(6 * T, H)] = (py[:H] + got(2, k, 0, H) + got(4, k)).astype(BF16)
        out[pl.ds(6 * T + H, H)] = (py[H:] + got(2, k, H, H)).astype(BF16)
        rs_copy(7, k).start()

    def out_copy(k):
        return pltpu.make_async_copy(
            xg.at[9, pl.ds((k % 2) * T, T)], y.at[:, pl.ds(pl.multiple_of(k * C, C), C)], out_sem.at[k % 2]
        )

    def finish(k):
        for kind in (3, 6, 7):
            rs_copy(kind, k).wait_recv()

        @pl.when(k >= 2)
        def _():
            out_copy(k - 2).wait()

        total = part(3, k)[...] + got(3, k) + got(6, k) + got(7, k)
        xg[9, pl.ds((k % 2) * T, T)] = total.astype(BF16)
        out_copy(k).start()

    def down_step(i, _):
        @pl.when(i < K)
        def _():
            compute(i)

        @pl.when((i >= 1) & (i <= K))
        def _():
            pass_on(i - 1)

        @pl.when(i >= 2)
        def _():
            finish(i - 2)
        return 0

    lax.fori_loop(0, K + 2, down_step, 0)
    for k in range(K - 2, K):
        out_copy(k).wait()
        for kind in range(8):
            rs_copy(kind, k).wait_send()
    for d in range(1, members):
        code_copy(d, pk, cg.at[me], mate).wait_send()


def solution(mesh):
    members = mesh.shape["ep"]

    def body(x, expert, slot, gate, w_gate, w_up, w_down, s_gate, s_up, s_down):
        local, depth, width = w_gate.shape
        tokens, top = expert.shape[2:]
        x, (expert, slot, gate) = x[0, 0], (jnp.transpose(v[0], (2, 0, 1)) for v in (expert, slot, gate))
        slots = 5 * tokens * top // (4 * members * local)
        chunks, parts = depth // C, width // C
        dims = (members, local, slots, top, chunks, parts)
        rows, M = local * slots, members * slots
        anywhere = pl.BlockSpec(memory_space=pl.ANY)
        dma = pltpu.SemaphoreType.DMA
        out = pl.pallas_call(
            functools.partial(moe_kernel, dims),
            out_shape=jax.ShapeDtypeStruct((tokens, depth), BF16),
            in_specs=[pl.BlockSpec(memory_space=pltpu.VMEM)] * 3 + [anywhere] * 7,
            out_specs=anywhere,
            scratch_shapes=[
                pltpu.VMEM((chunks, members * tokens, C), BF16),
                pltpu.VMEM((local, M, 2 * width), F32),
                pltpu.VMEM((UNITS, parts, C, C), BF16),
                pltpu.VMEM((parts, 2 * tokens, C), BF16),
                pltpu.VMEM((members * tokens, C), BF16),
                pltpu.VMEM((members, tokens, tokens), BF16),
                pltpu.VMEM((members, tokens, tokens), BF16),
                pltpu.VMEM((members, 16, tokens), F32),
                pltpu.VMEM((16, tokens), F32),
                dma((chunks,)), dma((members,)), dma((members,)),
                dma((9, chunks)), dma((9, chunks)), dma((UNITS,)),
                dma((8, 2)), dma((8, 4)), dma((2,)),
            ],
            compiler_params=pltpu.CompilerParams(
                collective_id=0, has_side_effects=True, vmem_limit_bytes=67_000_000
            ),
            name="moe",
        )(expert, slot, gate, x, w_gate, w_up, w_down, s_gate, s_up, s_down)
        return out[None, None]

    own = P("dp", "ep", None, None)
    experts, whole = P("ep", None, None), P(None, None)
    return jax.shard_map(
        body,
        mesh=mesh,
        in_specs=(own, own, own, own, experts, experts, experts, whole, whole, whole),
        out_specs=own,
        check_vma=False,
    )
```

```python
import functools

import jax
import jax.numpy as jnp
from jax import lax
from jax.experimental import pallas as pl
from jax.experimental.pallas import tpu as pltpu
from jax.sharding import PartitionSpec as P

F32, BF16 = jnp.float32, jnp.bfloat16
MESH = pl.DeviceIdType.MESH
C = 512
UNITS = 8


def dot(a, b):
    return jnp.dot(a, b, preferred_element_type=F32)


def moe_kernel(
    dims, expert, slot_of, gate, x, wg, wu, wd, sg, su, sd, y,
    xg, acc, ring, hs, zb, dm, wm, cg, pk,
    ld_sem, cg_send, cg_recv, ag_send, ag_recv, ring_sem, rs_send, rs_recv, out_sem,
):
    members, local, slots, top, chunks, parts = dims
    T = 256
    rows = local * slots
    M = members * slots
    K = chunks
    me = lax.axis_index("ep")
    core, yy, xx = me % 2, (me // 2) % 2, me // 4
    mate, ynbr, xnbr = me + 1 - 2 * core, me + 2 - 4 * yy, me + 4 - 8 * xx
    diag = ynbr + 4 - 8 * xx
    n_shared, n_routed, per_down = 2 * K, 2 * local * K, local + 1
    half = pl.multiple_of(core * parts * C, C)

    def unit_copy(src, r0, c0, down, n):
        slot = n % UNITS
        for j in range(parts):
            if down:
                piece = src.at[pl.ds(r0 + j * C, C), pl.ds(c0, C)]
            else:
                piece = src.at[pl.ds(r0, C), pl.ds(c0 + j * C, C)]
            pltpu.make_async_copy(piece, ring.at[slot, j], ring_sem.at[slot]).start(priority=1)

    def unit_wait(n):
        slot = n % UNITS
        pltpu.make_async_copy(ring.at[slot], ring.at[slot], ring_sem.at[slot]).wait()
        return slot

    def start_shared(i, t, n):
        unit_copy((sg, su)[t], pl.multiple_of(i * C, C), half, False, n)

    def start_routed(k, q, n):
        w = wg if q % 2 == 0 else wu
        unit_copy(w.at[q // 2], pl.multiple_of(k * C, C), 0, False, n)

    def start_down(k, m, n):
        c0 = pl.multiple_of(k * C, C)
        if m < local:
            unit_copy(wd.at[m], 0, c0, True, n)
        else:
            unit_copy(sd, half, c0, True, n)

    def blk(k, s, off=0, n=T):
        return xg.at[k, pl.ds(pl.multiple_of(s * T + off, 128), n)]

    H = T // 2
    routes = (
        (me, 0, T, xnbr), (me, 0, T, ynbr), (me, 0, T, mate),
        (xnbr, 0, H, ynbr), (ynbr, H, H, xnbr),
        (xnbr, 0, T, mate), (ynbr, 0, T, mate), (diag, 0, H, mate), (diag, H, H, mate),
    )
    mx, my, md = mate + 4 - 8 * xx, mate + 2 - 4 * yy, mate + 2 - 4 * yy + 4 - 8 * xx
    landed = (
        (xnbr, 0, T), (ynbr, 0, T), (mate, 0, T), (diag, 0, H), (diag, H, H),
        (mx, 0, T), (my, 0, T), (md, 0, H), (md, H, H),
    )

    def route(kind, k, ref, dev):
        return pltpu.make_async_remote_copy(
            src_ref=ref, dst_ref=ref, send_sem=ag_send.at[kind, k], recv_sem=ag_recv.at[kind, k],
            device_id={"ep": dev}, device_id_type=MESH,
        )

    def ag_start(kinds, k):
        for kind in kinds:
            s, off, n, dev = routes[kind]
            route(kind, k, blk(k, s, off, n), dev).start()

    def ag_sent(kinds, k):
        for kind in kinds:
            s, off, n, dev = routes[kind]
            route(kind, k, blk(k, s, off, n), dev).wait_send()

    def ag_wait(kinds, k):
        for kind in kinds:
            s, off, n = landed[kind]
            route(kind, k, blk(k, s, off, n), mate).wait_recv()

    def comm_a(k):
        ag_wait((0, 1), k)

        @pl.when(k >= 2)
        def _():
            ag_sent(range(9), k - 2)

        ag_start((3, 4, 5, 6), k)

        @pl.when(k + 2 < K)
        def _():
            ag_start((0, 1), k + 2)

    def comm_b(k):
        ag_wait((3, 4), k)
        ag_start((7, 8), k)

    def own_load(k):
        return pltpu.make_async_copy(x.at[:, pl.ds(pl.multiple_of(k * C, C), C)], blk(k, me), ld_sem.at[k])

    for k in range(K):
        own_load(k).start()
    for n in range(UNITS):
        start_shared(n // 2, n % 2, n)
    pk[...] = jnp.zeros(pk.shape, F32)
    for j in range(top):
        place = slot_of[j]
        pk[j:j + 1] = jnp.where(place < slots, expert[j] * slots + place, -1).astype(F32)
        pk[8 + j:9 + j] = gate[j].astype(BF16).astype(F32)
    barrier = pltpu.get_barrier_semaphore()
    for d in range(1, members):
        pl.semaphore_signal(barrier, inc=1, device_id={"ep": (me + d) % members}, device_id_type=MESH)
    pl.semaphore_wait(barrier, members - 1)

    def code_copy(d, src, dst, dev):
        return pltpu.make_async_remote_copy(
            src_ref=src, dst_ref=dst, send_sem=cg_send.at[d], recv_sem=cg_recv.at[d],
            device_id={"ep": dev}, device_id_type=MESH,
        )

    own_load(0).wait()
    ag_start((0, 1, 2), 0)
    for d in range(1, members):
        code_copy(d, pk, cg.at[me], (me + d) % members).start()
    own_load(1).wait()
    ag_start((0, 1, 2), 1)
    cg[me] = pk[...]

    for k in range(2, K):
        own_load(k).wait()
        ag_start((2,), k)
    zb[pl.ds(local * M, members * T - local * M)] = jnp.zeros((members * T - local * M, C), BF16)

    def tables(s):
        codes = cg[s]
        row = lax.broadcasted_iota(jnp.int32, (T, T), 0)
        row = jnp.where(row < rows, row + me * rows, -2).astype(F32)
        hit = jnp.zeros((T, T), F32)
        weight = jnp.zeros((T, T), F32)
        for j in range(top):
            same = codes[j:j + 1, :] == row
            hit = jnp.where(same, 1.0, hit)
            weight = jnp.where(same, codes[8 + j:9 + j, :], weight)
        dm[s] = hit.astype(BF16)
        wm[s] = weight.T.astype(BF16)

    def shared_step(i, _):
        ag_wait((2,), i)
        held = [unit_wait(2 * i + t) for t in range(2)]
        both = xg[i, pl.ds(pl.multiple_of((me - core) * T, 2 * T), 2 * T)]
        for t in range(2):
            for j in range(parts):
                cols = pl.ds((t * parts + j) * C, C)
                term = dot(both, ring[held[t], j])
                acc[3, :T, cols] = jnp.where(i > 0, acc[3, :T, cols], 0.0) + term[:T]
                acc[4, :T, cols] = jnp.where(i > 0, acc[4, :T, cols], 0.0) + term[T:]

        @pl.when(i < K - 4)
        def _():
            for t in range(2):
                start_shared(i + 4, t, 2 * i + t + UNITS)

        for late in range(4):
            @pl.when(i == K - 4 + late)
            def _():
                for t in range(2):
                    start_routed(0, 2 * late + t, 2 * i + t + UNITS)

        @pl.when(i == 1)
        def _():
            for d in range(1, members):
                code_copy(d, pk, cg.at[(me + members - d) % members], mate).wait_recv()

        @pl.when(i >= 2)
        def _():
            tables(i - 2)

        @pl.when(i == 3)
        def _():
            comm_a(0)

        @pl.when(i == 7)
        def _():
            comm_a(1)
        return 0

    lax.fori_loop(0, K, shared_step, 0)
    for side in range(2):
        for j in range(parts):
            g = acc[3 + side, :T, pl.ds(j * C, C)]
            u = acc[3 + side, :T, pl.ds((parts + j) * C, C)]
            hs[j, pl.ds(side * T, T)] = (jax.nn.silu(g) * u).astype(BF16)
    comm_b(0)

    def hidden(e):
        for j in range(parts):
            g = acc[e, :, pl.ds(j * C, C)]
            u = acc[e, :, pl.ds((parts + j) * C, C)]
            xg[6 + j, pl.ds(e * M, M)] = (jax.nn.silu(g) * u).astype(BF16)

    groups = [[0], list(range(1, local - 2)), [local - 2, local - 1]]

    def routed_step(k, last):
        base = n_shared + 2 * local * k
        ag_wait((5, 6, 7, 8), k)
        for group in groups:
            units = [2 * e + t for e in group for t in range(2)]
            held = [unit_wait(base + q) for q in units]
            if group[0] == 0:
                for s in range(members):
                    z = dot(dm[s, :rows], xg[k, pl.ds(s * T, T)]).astype(BF16)
                    for e in range(local):
                        zb[pl.ds(e * M + s * slots, slots)] = z[e * slots:(e + 1) * slots]
            elif last:
                hidden(group[0] - 1)
            for e in group:
                z = zb[pl.ds(e * M, M)]
                for t in range(2):
                    for j in range(parts):
                        cols = pl.ds((t * parts + j) * C, C)
                        old = acc[e, :, cols]
                        if not last:
                            old = jnp.where(k > 0, old, 0.0)
                        acc[e, :, cols] = old + dot(z, ring[held[units.index(2 * e + t)], j])
                if last and e != group[-1]:
                    hidden(e)
            for q in units:
                ahead = q + UNITS
                if ahead < 2 * local:
                    start_routed(k, ahead, base + q + UNITS)
                elif not last:
                    start_routed(k + 1, ahead - 2 * local, base + q + UNITS)
                else:
                    ahead -= 2 * local
                    start_down(ahead // per_down, ahead % per_down, base + q + UNITS)
            if group is groups[0] and not last:
                @pl.when(k + 2 < K)
                def _():
                    comm_a(k + 2)
            if group is groups[1] and not last:
                comm_b(k + 1)
        return 0

    lax.fori_loop(0, K - 1, lambda k, _: routed_step(k, False), 0)
    ag_sent(range(9), K - 2)
    routed_step(K - 1, True)
    hidden(groups[-1][-1])
    ag_sent(range(9), K - 1)

    spans = ((0, T), (T, T), (2 * T, T), (3 * T, T), (4 * T, H), (4 * T + H, H), (5 * T, T), (6 * T, T))
    targets = (mate, mate, mate, mate, xnbr, ynbr, xnbr, ynbr)
    mine, theirs = (diag, xnbr, ynbr, me), (md, mx, my, mate)

    def rs_copy(kind, k):
        off, n = spans[kind]
        return pltpu.make_async_remote_copy(
            src_ref=xg.at[4 + k % 2, pl.ds(off, n)], dst_ref=xg.at[k % 4, pl.ds(off, n)],
            send_sem=rs_send.at[kind, k % 2], recv_sem=rs_recv.at[kind, k % 4],
            device_id={"ep": targets[kind]}, device_id_type=MESH,
        )

    def rs_free(kinds, k):
        @pl.when(k >= 2)
        def _():
            for kind in kinds:
                rs_copy(kind, k - 2).wait_send()

    def got(kind, k, lo=0, n=None):
        off, size = spans[kind]
        return xg[k % 4, pl.ds(off + lo, size if n is None else n)].astype(F32)

    def part(r, k):
        return acc.at[k % 4, pl.ds(0, T), pl.ds(r * C, C)]

    def compute(k):
        base = n_shared + n_routed + per_down * k

        def refill(ms):
            for ks in (1, 2):
                some = [m for m in ms if (m + UNITS) // per_down == ks]
                if some:
                    @pl.when(k + ks < K)
                    def _():
                        for m in some:
                            start_down(k + ks, (m + UNITS) % per_down, base + m + UNITS)

        for group in (range(3), range(3, per_down)):
            held = [unit_wait(base + m) for m in group]
            for slot, e in zip(held, group):
                if e == local:
                    continue
                out = dot(xg[6, pl.ds(e * M, M)], ring[slot, 0])
                for j in range(1, parts):
                    out = out + dot(xg[6 + j, pl.ds(e * M, M)], ring[slot, j])
                out = out.astype(BF16)
                for s in range(members):
                    zb[pl.ds(s * T + e * slots, slots)] = out[s * slots:(s + 1) * slots]
            refill([m for m in group if m < local])
        shared = held[-1]

        def combined(s):
            return dot(wm[s], zb[pl.ds(pl.multiple_of(s * T, T), T)])

        def shared_part(side):
            total = None
            for j in range(parts):
                term = dot(hs[j, pl.ds(pl.multiple_of(side * T, T), T)], ring[shared, j])
                total = term if total is None else total + term
            return total

        def send(r, p):
            xg[4 + k % 2, pl.ds(r * T, T)] = p.astype(BF16)
            rs_copy(r, k).start()

        rs_free(range(4), k)
        for r in range(3):
            send(r, combined(theirs[r]))
        for r in range(3):
            part(r, k)[...] = combined(mine[r])
        rs_copy(0, k).wait_recv()
        rs_free((4, 5), k)
        xg[4 + k % 2, pl.ds(4 * T, T)] = (part(0, k)[...] + got(0, k)).astype(BF16)
        rs_copy(4, k).start()
        rs_copy(5, k).start()
        send(3, combined(theirs[3]) + shared_part(1 - core))
        part(3, k)[...] = combined(mine[3]) + shared_part(core)
        refill([local])

    def pass_on(k):
        for kind in (1, 2, 4, 5):
            rs_copy(kind, k).wait_recv()
        rs_free((6, 7), k)
        out = xg.at[4 + k % 2]
        px, py = part(1, k), part(2, k)
        out[pl.ds(5 * T, H)] = (px[:H] + got(1, k, 0, H)).astype(BF16)
        out[pl.ds(5 * T + H, H)] = (px[H:] + got(1, k, H, H) + got(5, k)).astype(BF16)
        rs_copy(6, k).start()
        out[pl.ds(6 * T, H)] = (py[:H] + got(2, k, 0, H) + got(4, k)).astype(BF16)
        out[pl.ds(6 * T + H, H)] = (py[H:] + got(2, k, H, H)).astype(BF16)
        rs_copy(7, k).start()

    def out_copy(k):
        return pltpu.make_async_copy(
            xg.at[9, pl.ds((k % 2) * T, T)], y.at[:, pl.ds(pl.multiple_of(k * C, C), C)], out_sem.at[k % 2]
        )

    def finish(k):
        for kind in (3, 6, 7):
            rs_copy(kind, k).wait_recv()

        @pl.when(k >= 2)
        def _():
            out_copy(k - 2).wait()

        total = part(3, k)[...] + got(3, k) + got(6, k) + got(7, k)
        xg[9, pl.ds((k % 2) * T, T)] = total.astype(BF16)
        out_copy(k).start()

    def down_step(i, _):
        @pl.when(i < K)
        def _():
            compute(i)

        @pl.when((i >= 1) & (i <= K))
        def _():
            pass_on(i - 1)

        @pl.when(i >= 2)
        def _():
            finish(i - 2)
        return 0

    lax.fori_loop(0, K + 2, down_step, 0)
    for k in range(K - 2, K):
        out_copy(k).wait()
        for kind in range(8):
            rs_copy(kind, k).wait_send()
    for d in range(1, members):
        code_copy(d, pk, cg.at[me], mate).wait_send()


def solution(mesh):
    members = mesh.shape["ep"]

    def body(x, expert, slot, gate, w_gate, w_up, w_down, s_gate, s_up, s_down):
        local, depth, width = w_gate.shape
        tokens, top = expert.shape[2:]
        x, (expert, slot, gate) = x[0, 0], (jnp.transpose(v[0], (2, 0, 1)) for v in (expert, slot, gate))
        slots = 5 * tokens * top // (4 * members * local)
        chunks, parts = depth // C, width // C
        dims = (members, local, slots, top, chunks, parts)
        rows, M = local * slots, members * slots
        anywhere = pl.BlockSpec(memory_space=pl.ANY)
        dma = pltpu.SemaphoreType.DMA
        out = pl.pallas_call(
            functools.partial(moe_kernel, dims),
            out_shape=jax.ShapeDtypeStruct((tokens, depth), BF16),
            in_specs=[pl.BlockSpec(memory_space=pltpu.VMEM)] * 3 + [anywhere] * 7,
            out_specs=anywhere,
            scratch_shapes=[
                pltpu.VMEM((chunks, members * tokens, C), BF16),
                pltpu.VMEM((local, M, 2 * width), F32),
                pltpu.VMEM((UNITS, parts, C, C), BF16),
                pltpu.VMEM((parts, 2 * tokens, C), BF16),
                pltpu.VMEM((members * tokens, C), BF16),
                pltpu.VMEM((members, tokens, tokens), BF16),
                pltpu.VMEM((members, tokens, tokens), BF16),
                pltpu.VMEM((members, 16, tokens), F32),
                pltpu.VMEM((16, tokens), F32),
                dma((chunks,)), dma((members,)), dma((members,)),
                dma((9, chunks)), dma((9, chunks)), dma((UNITS,)),
                dma((8, 2)), dma((8, 4)), dma((2,)),
            ],
            compiler_params=pltpu.CompilerParams(
                collective_id=0, has_side_effects=True, vmem_limit_bytes=67_000_000
            ),
            name="moe",
        )(expert, slot, gate, x, w_gate, w_up, w_down, s_gate, s_up, s_down)
        return out[None, None]

    own = P("dp", "ep", None, None)
    experts, whole = P("ep", None, None), P(None, None)
    return jax.shard_map(
        body,
        mesh=mesh,
        in_specs=(own, own, own, own, experts, experts, experts, whole, whole, whole),
        out_specs=own,
        check_vma=False,
    )
```
